32 devices in a mesh: dp: 4 (over x, y), tp: 8 (over z, core).
Axes of the slice: x: 2, y: 2, z: 4, core: 2. Of those that a mesh axis runs over, the one named last changes fastest.
Arguments:
- x: bfloat16 [8192, 8192], P('dp'), parts along dimension 0
- w_gate: bfloat16 [8192, 24576], P(None, 'tp')
- w_up: bfloat16 [8192, 24576], P(None, 'tp')
- w_down: bfloat16 [24576, 8192], P('tp')
Outputs:
- output: bfloat16 [8192, 8192], P('dp'), parts along dimension 0
There are 4 independent parts. The reference program is written for one: setup_inputs(seed, part) draws one part's arguments, and reference() takes and returns one part's arrays. A program takes and returns all parts, laid end to end along the dimension named above; an argument that names none is the same for every part.
All inputs are finite; a program needn't handle non-finite values.
Results may differ from the reference program's by a relative error of at most 0.016.
Values are sent between devices in bfloat16 or wider.
A program may use at most 2 GiB of HBM per device.

```python
import jax
import jax.numpy as jnp

ROWS = 2048
D = 8192
FF = 24576


def setup_inputs(seed: int = 0, part: int = 0) -> dict:
    kx, kg, ku, kd = jax.random.split(jax.random.key(seed), 4)
    drawn = {
        "x": jax.random.normal(jax.random.fold_in(kx, part), (ROWS, D), jnp.float32),
        "w_gate": jax.random.normal(kg, (D, FF), jnp.float32) * D**-0.5,
        "w_up": jax.random.normal(ku, (D, FF), jnp.float32) * D**-0.5,
        "w_down": jax.random.normal(kd, (FF, D), jnp.float32) * FF**-0.5,
    }
    return {k: v.astype(jnp.bfloat16) for k, v in drawn.items()}


def reference(x, w_gate, w_up, w_down):
    gate = jnp.dot(x, w_gate, preferred_element_type=jnp.float32)
    up = jnp.dot(x, w_up, preferred_element_type=jnp.float32)
    hidden = (jax.nn.silu(gate) * up).astype(jnp.bfloat16)
    return jnp.dot(hidden, w_down, preferred_element_type=jnp.float32).astype(jnp.bfloat16)
```

```python
import functools

import jax
import jax.numpy as jnp
from jax import lax
from jax.experimental import pallas as pl
from jax.experimental.pallas import tpu as pltpu
from jax.sharding import PartitionSpec as P

MESH = pl.DeviceIdType.MESH
BF16, F32 = jnp.bfloat16, jnp.float32
BLOCK, CHUNK, NA = 512, 128, 256
VMEM = 67043328
LAGS = (1, 3, 5, 7)


def kernel(
    x, wg, wu, wd,
    y, cin, xin,
    xb, hb, wa, wb, part, sent, psend, pbuf, cload, xload, xsend, tsend,
    sx, sa, sb, p_send, p_recv, p_free, o_send, c_recv, x_send, x_recv,
    t_send, y_recv, f_send, g_send, yp_recv, l_sem,
):
    rows, d = x.shape
    ff = wg.shape[1]
    half, nb = d // 2, d // 8
    hw = nb // 2
    steps_a, blocks, per = ff // NA, rows // BLOCK, BLOCK // CHUNK
    chunks = blocks * 4 * per
    d1, d2, d3, d4 = LAGS

    dp, me = lax.axis_index("dp"), lax.axis_index("tp")
    z, c = me // 2, me % 2
    inner = (z == 1) | (z == 2)
    outer = jnp.logical_not(inner)
    partner = me + 1 - 2 * c
    inward = (1 + z // 2) * 2 + c
    outward = (3 * (z - 1)) * 2 + c
    across = (3 - z) * 2 + c
    mine = pl.multiple_of(jnp.where(z == 2, hw, 0), hw)
    other = pl.multiple_of(hw - mine, hw)
    own0, par0 = c * half, (1 - c) * half

    def remote(src, dst, send, recv, to):
        return pltpu.make_async_remote_copy(
            src_ref=src, dst_ref=dst, send_sem=send, recv_sem=recv,
            device_id=(dp, to), device_id_type=MESH,
        )

    def place(u):
        b, i, r = u // (4 * per), (u // per) % 4, u % per
        return pl.ds(pl.multiple_of(b * BLOCK + r * CHUNK, CHUNK), CHUNK), i, pl.ds(pl.multiple_of(r * CHUNK, CHUNK), CHUNK)

    def cols(base, i, off, n):
        return pl.ds(pl.multiple_of(base + i * nb + off, n), n)

    def x_copy(b):
        return pltpu.make_async_copy(x.at[pl.ds(pl.multiple_of(b * BLOCK, BLOCK), BLOCK), :], xb, sx)

    def a_copies(n, s):
        col = pl.ds(pl.multiple_of(n * NA, NA), NA)
        return [pltpu.make_async_copy(w.at[:, col], wa.at[s, j], sa.at[s, j]) for j, w in enumerate((wg, wu))]

    def b_copy(base, i, s):
        return pltpu.make_async_copy(wd.at[:, cols(base, i, 0, nb)], wb.at[s], sb.at[s])

    def p_copy():
        return remote(psend, pbuf, p_send, p_recv, partner)

    def o_copy(b, i, r):
        rw = pl.ds(pl.multiple_of(b * BLOCK + r * CHUNK, CHUNK), CHUNK)
        return remote(
            sent.at[i, pl.ds(r * CHUNK, CHUNK), :], cin.at[rw, cols(0, i, 0, nb)],
            o_send.at[i], c_recv.at[(b * 4 + i) * per + r], inward,
        )

    def o_wait(i):
        remote(sent.at[i], cin.at[pl.ds(0, BLOCK), cols(0, i, 0, nb)], o_send.at[i], c_recv.at[0], inward).wait_send()

    def c_arrival(u):
        rw, i, _ = place(u)
        return remote(cin.at[rw, cols(0, i, 0, nb)], cin.at[rw, cols(0, i, 0, nb)], o_send.at[0], c_recv.at[u], outward)

    def c_load(u):
        rw, i, _ = place(u)
        return pltpu.make_async_copy(cin.at[rw, cols(0, i, 0, nb)], cload, l_sem.at[0])

    def x_cols(i):
        return pl.ds(pl.multiple_of(i * hw, hw), hw)

    def e_copy(u):
        rw, i, _ = place(u)
        return remote(xsend.at[u % 4], xin.at[rw, x_cols(i)], x_send.at[u % 4], x_recv.at[u], across)

    def x_load(u):
        rw, i, _ = place(u)
        return pltpu.make_async_copy(xin.at[rw, x_cols(i)], xload, l_sem.at[1])

    def t_copies(u):
        rw, i, _ = place(u)
        dst, s = y.at[rw, cols(own0, i, mine, hw)], u % 4
        src = tsend.at[s]
        return [
            remote(src, dst, t_send.at[s, 0], y_recv.at[0, u], outward),
            remote(src, dst, t_send.at[s, 1], y_recv.at[0, u], across),
            remote(src, dst, t_send.at[s, 2], yp_recv, partner),
            pltpu.make_async_copy(src, dst, t_send.at[s, 3]),
        ]

    def t_wait(u):
        for j, t in enumerate(t_copies(u)):
            t.wait_send() if j < 3 else t.wait()

    def hand_on(u):
        rw, i, _ = place(u)
        at = y.at[rw, cols(own0, i, other, hw)]
        return remote(at, at, f_send, y_recv.at[1, u], outward), remote(at, at, g_send, yp_recv, partner)

    def pass_over(u):
        rw, i, _ = place(u)
        at = y.at[rw, cols(own0, i, 0, nb)]
        return remote(at, at, g_send, yp_recv, partner)

    def y_arrival(u, kind, off):
        rw, i, _ = place(u)
        at = y.at[rw, cols(own0, i, off, hw)]
        return remote(at, at, f_send, y_recv.at[kind, u], across)

    def live(u):
        return (u >= 0) & (u < chunks)

    def before(k):
        u, v = k - d1, k - d2

        @pl.when(inner & live(u))
        def _():
            c_arrival(u).wait_recv()
            c_load(u).start()

        @pl.when(inner & live(v))
        def _():
            e_copy(v).wait_recv()
            x_load(v).start()

    def after(k):
        u, v, w, q = k - d1, k - d2, k - d3, k - d4

        @pl.when(inner & live(u))
        def _():
            @pl.when(u >= 4)
            def _():
                e_copy(u - 4).wait_send()

            _, i, r = place(u)
            c_load(u).wait()
            xsend[u % 4] = (part[i, r, pl.ds(other, hw)] + cload[:, pl.ds(other, hw)].astype(F32)).astype(BF16)
            e_copy(u).start()
            part[i, r, pl.ds(mine, hw)] += cload[:, pl.ds(mine, hw)].astype(F32)

        @pl.when(inner & live(v))
        def _():
            @pl.when(v >= 4)
            def _():
                t_wait(v - 4)

            _, i, r = place(v)
            x_load(v).wait()
            tsend[v % 4] = (part[i, r, pl.ds(mine, hw)] + xload[...].astype(F32)).astype(BF16)
            for t in t_copies(v):
                t.start()

        @pl.when(inner & live(w))
        def _():
            y_arrival(w, 0, other).wait_recv()
            for t in hand_on(w):
                t.start()

        @pl.when(outer & live(q))
        def _():
            near = pl.multiple_of(jnp.where(z == 3, hw, 0), hw)
            y_arrival(q, 0, near).wait_recv()
            y_arrival(q, 1, pl.multiple_of(hw - near, hw)).wait_recv()
            pass_over(q).start()

    barrier = pltpu.get_barrier_semaphore()
    pl.semaphore_signal(barrier, inc=1, device_id=(dp, partner), device_id_type=MESH)

    @pl.when(inner)
    def _():
        pl.semaphore_signal(barrier, inc=1, device_id=(dp, outward), device_id_type=MESH)
        pl.semaphore_signal(barrier, inc=1, device_id=(dp, across), device_id_type=MESH)
        pl.semaphore_wait(barrier, 3)

    @pl.when(outer)
    def _():
        pl.semaphore_signal(barrier, inc=1, device_id=(dp, inward), device_id_type=MESH)
        pl.semaphore_wait(barrier, 2)

    x_copy(0).start()
    for t in a_copies(0, 0):
        t.start()

    def block(b, _):
        x_copy(b).wait()

        def a_step(n, _):
            s, k = n % 2, b * 4 * per - steps_a + n

            @pl.when(n + 1 < steps_a)
            def _():
                for t in a_copies(n + 1, 1 - s):
                    t.start()

            @pl.when(n == steps_a - 1)
            def _():
                b_copy(par0, 0, 0).start()

            before(k)
            for t in a_copies(n, s):
                t.wait()
            gate = jnp.dot(xb[...], wa[s, 0], preferred_element_type=F32)
            up = jnp.dot(xb[...], wa[s, 1], preferred_element_type=F32)
            hb[:, pl.ds(pl.multiple_of(n * NA, NA), NA)] = (jax.nn.silu(gate) * up).astype(BF16)
            after(k)
            return 0

        lax.fori_loop(0, steps_a, a_step, 0)

        def b_step(i, _):
            k = b * 4 * per + i
            b_copy(own0, i, 1).start()

            @pl.when((i == 0) & (b + 1 < blocks))
            def _():
                x_copy(b + 1).start()

            b_copy(par0, i, 0).wait()
            count = b * 4 + i

            @pl.when(count > 0)
            def _():
                p_copy().wait_send()

            psend[...] = jnp.dot(hb[...], wb[0], preferred_element_type=F32).astype(BF16)

            @pl.when(count > 0)
            def _():
                pl.semaphore_wait(p_free, 1)

            p_copy().start()

            @pl.when(i < 3)
            def _():
                b_copy(par0, i + 1, 0).start()

            @pl.when((i == 3) & (b + 1 < blocks))
            def _():
                for t in a_copies(0, 0):
                    t.start()

            before(k)
            b_copy(own0, i, 1).wait()
            part[i] = jnp.dot(hb[...], wb[1], preferred_element_type=F32)
            p_copy().wait_recv()

            @pl.when(inner)
            def _():
                part[i] += pbuf[...].astype(F32)

            @pl.when(outer)
            def _():
                @pl.when(b > 0)
                def _():
                    o_wait(i)

                for r in range(per):
                    at = pl.ds(r * CHUNK, CHUNK)
                    sent[i, at, :] = (part[i, at, :] + pbuf[at, :].astype(F32)).astype(BF16)
                    o_copy(b, i, r).start()

            @pl.when(count < blocks * 4 - 1)
            def _():
                pl.semaphore_signal(p_free, inc=1, device_id=(dp, partner), device_id_type=MESH)

            after(k)
            return 0

        lax.fori_loop(0, 4, b_step, 0)
        return 0

    lax.fori_loop(0, blocks, block, 0)

    def drain(k, _):
        before(k)
        after(k)
        return 0

    lax.fori_loop(chunks - 4 * per + 4, chunks + d4, drain, 0)

    p_copy().wait_send()
    side = y.at[:, pl.ds(0, half)]
    quarter = y.at[:, pl.ds(0, half // 2)]

    @pl.when(outer)
    def _():
        for i in range(4):
            o_wait(i)
        remote(side, side, g_send, yp_recv, partner).wait_send()

    @pl.when(inner)
    def _():
        for s in range(4):
            e_copy(chunks - 4 + s).wait_send()
            t_wait(chunks - 4 + s)
        remote(quarter, quarter, f_send, yp_recv, partner).wait_send()
        remote(quarter, quarter, g_send, yp_recv, partner).wait_send()

    remote(side, side, g_send, yp_recv, partner).wait_recv()


def block_call(x, wg, wu, wd):
    rows, d = x.shape
    ff = wg.shape[1]
    half, nb = d // 2, d // 8
    hw = nb // 2
    chunks = (rows // BLOCK) * 4 * (BLOCK // CHUNK)
    dma, any_ = pltpu.SemaphoreType.DMA, pl.BlockSpec(memory_space=pl.ANY)
    flops = 6 * rows * d * ff
    return pl.pallas_call(
        kernel,
        out_shape=[
            jax.ShapeDtypeStruct((rows, d), BF16),
            jax.ShapeDtypeStruct((rows, half), BF16),
            jax.ShapeDtypeStruct((rows, half // 2), BF16),
        ],
        in_specs=[any_] * 4,
        out_specs=[any_] * 3,
        scratch_shapes=[
            pltpu.VMEM((BLOCK, d), BF16),
            pltpu.VMEM((BLOCK, ff), BF16),
            pltpu.VMEM((2, 2, d, NA), BF16),
            pltpu.VMEM((2, ff, nb), BF16),
            pltpu.VMEM((4, BLOCK, nb), F32),
            pltpu.VMEM((4, BLOCK, nb), BF16),
            pltpu.VMEM((BLOCK, nb), BF16),
            pltpu.VMEM((BLOCK, nb), BF16),
            pltpu.VMEM((CHUNK, nb), BF16),
            pltpu.VMEM((CHUNK, hw), BF16),
            pltpu.VMEM((4, CHUNK, hw), BF16),
            pltpu.VMEM((4, CHUNK, hw), BF16),
            dma, dma((2, 2)), dma((2,)), dma, dma, pltpu.SemaphoreType.REGULAR,
            dma((4,)), dma((chunks,)), dma((4,)), dma((chunks,)),
            dma((4, 4)), dma((2, chunks)), dma, dma, dma, dma((2,)),
        ],
        compiler_params=pltpu.CompilerParams(collective_id=0, has_side_effects=True, vmem_limit_bytes=VMEM),
        cost_estimate=pl.CostEstimate(flops=flops, bytes_accessed=10**9, transcendentals=rows * ff),
        name="mlp_block",
    )(x, wg, wu, wd)[0]


def solution(mesh):
    return jax.shard_map(
        block_call,
        mesh=mesh,
        in_specs=(P("dp", None), P(None, "tp"), P(None, "tp"), P("tp", None)),
        out_specs=P("dp", None),
        check_vma=False,
    )
```

```python
import functools

import jax
import jax.numpy as jnp
from jax import lax
from jax.experimental import pallas as pl
from jax.experimental.pallas import tpu as pltpu
from jax.sharding import PartitionSpec as P

MESH = pl.DeviceIdType.MESH
BF16, F32 = jnp.bfloat16, jnp.float32
BLOCK, CHUNK, NA = 384, 128, 256
BULK = 1
VMEM = 67043328
SLOTS, RING, DEEP = 8, 4, 3
STEP_A, STEP_B, DUE = 184, 144, 630
LAGS, BEHIND = (0, 2, 5), 16


def kernel(
    x, wg, wu, wd,
    y, cin,
    xb, hb, wa, wb, part, sent, psend, pbuf, cload, xin, xsend, tsend,
    sx, sa, sb, p_send, p_recv, p_free, o_send, c_recv, x_send, x_recv,
    t_send, y_recv, f_send, g_send, yp_recv, l_sem,
):
    rows, d = x.shape
    ff = wg.shape[1]
    half, nb = d // 2, d // 8
    hw = nb // 2
    steps_a, whole, per = ff // NA, rows // BLOCK, BLOCK // CHUNK
    tail = rows - whole * BLOCK
    blocks, chunks, per_tail = whole + (tail > 0), rows // CHUNK * 4, max(tail // CHUNK, 1)
    tick = (8 * STEP_B + steps_a * STEP_A) // (4 * per)

    dp, me = lax.axis_index("dp"), lax.axis_index("tp")
    z, c = me // 2, me % 2
    inner = (z == 1) | (z == 2)
    outer = jnp.logical_not(inner)
    partner = me + 1 - 2 * c
    inward = (1 + z // 2) * 2 + c
    outward = (3 * (z - 1)) * 2 + c
    across = (3 - z) * 2 + c
    mine = pl.multiple_of(jnp.where(z == 2, hw, 0), hw)
    other = pl.multiple_of(hw - mine, hw)
    own0, par0 = c * half, (1 - c) * half

    def remote(src, dst, send, recv, to):
        return pltpu.make_async_remote_copy(
            src_ref=src, dst_ref=dst, send_sem=send, recv_sem=recv,
            device_id=(dp, to), device_id_type=MESH,
        )

    def place(u):
        b, w = lax.div(u, 4 * per), lax.rem(u, 4 * per)
        n = jnp.where(b < whole, per, per_tail)
        i = jnp.where(b < whole, lax.div(w, per), lax.div(w, per_tail))
        r = w - i * n
        return (
            pl.ds(pl.multiple_of(b * BLOCK + r * CHUNK, CHUNK), CHUNK), i, pl.ds(pl.multiple_of(r * CHUNK, CHUNK), CHUNK)
        )

    def cols(base, i, off, n):
        return pl.ds(pl.multiple_of(base + i * nb + off, n), n)

    def x_copy(b, m):
        return pltpu.make_async_copy(x.at[pl.ds(pl.multiple_of(b * BLOCK, CHUNK), m), :], xb.at[pl.ds(0, m), :], sx)

    def a_copies(n, s):
        col = pl.ds(pl.multiple_of(n * NA, NA), NA)
        return [pltpu.make_async_copy(w.at[:, col], wa.at[s, j], sa.at[s, j]) for j, w in enumerate((wg, wu))]

    def b_copy(base, i, s):
        return pltpu.make_async_copy(wd.at[:, cols(base, i, 0, nb)], wb.at[s], sb.at[s])

    def p_copy(m):
        return remote(psend.at[pl.ds(0, m), :], pbuf.at[pl.ds(0, m), :], p_send, p_recv, partner)

    def o_copy(b, i, r, u):
        rw = pl.ds(pl.multiple_of(b * BLOCK + r * CHUNK, CHUNK), CHUNK)
        return remote(
            sent.at[i, pl.ds(r * CHUNK, CHUNK), :], cin.at[rw, cols(0, i, 0, nb)],
            o_send.at[i], c_recv.at[u], inward,
        )

    def o_wait(i, m):
        at = pl.ds(0, m)
        remote(sent.at[i, at, :], cin.at[at, cols(0, i, 0, nb)], o_send.at[i], c_recv.at[0], inward).wait_send()

    def c_arrival(u):
        rw, i, _ = place(u)
        return remote(cin.at[rw, cols(0, i, 0, nb)], cin.at[rw, cols(0, i, 0, nb)], o_send.at[0], c_recv.at[u], outward)

    def c_load(u):
        rw, i, _ = place(u)
        return pltpu.make_async_copy(cin.at[rw, cols(0, i, 0, nb)], cload.at[lax.rem(u, 2)], l_sem.at[lax.rem(u, 2)])

    def e_copy(u):
        return remote(xsend.at[lax.rem(u, RING)], xin.at[lax.rem(u, SLOTS)], x_send.at[lax.rem(u, RING)], x_recv.at[lax.rem(u, SLOTS)], across)

    def t_copies(u):
        rw, i, _ = place(u)
        dst, s = y.at[rw, cols(own0, i, mine, hw)], lax.rem(u, RING)
        src = tsend.at[s]
        return [
            remote(src, dst, t_send.at[s, 0], y_recv.at[0, u], outward),
            remote(src, dst, t_send.at[s, 1], y_recv.at[0, u], across),
            remote(src, dst, t_send.at[s, 2], yp_recv, partner),
            pltpu.make_async_copy(src, dst, t_send.at[s, 3]),
        ]

    def t_wait(u):
        for j, t in enumerate(t_copies(u)):
            t.wait_send() if j < 3 else t.wait()

    def hand_on(u):
        rw, i, _ = place(u)
        at = y.at[rw, cols(own0, i, other, hw)]
        return remote(at, at, f_send, y_recv.at[1, u], outward), remote(at, at, g_send, yp_recv, partner)

    def pass_over(u):
        rw, i, _ = place(u)
        at = y.at[rw, cols(own0, i, 0, nb)]
        return remote(at, at, g_send, yp_recv, partner)

    def y_arrival(u, kind, off):
        rw, i, _ = place(u)
        at = y.at[rw, cols(own0, i, off, hw)]
        return remote(at, at, f_send, y_recv.at[kind, u], across)

    def advance(clock, step):
        t, due, *made = clock
        t = t + step
        on = jnp.where(t >= due, 1, 0)
        return (t, due + tick * on, made[0] + on, *made[:-1])

    def turn(clock, stage):
        made = clock[2:]
        lag, behind = (LAGS[stage], 0) if stage < 3 else (0, BEHIND)
        u = made[lag + 1] - behind
        return u, (made[lag] > made[lag + 1]) & (u >= 0) & (u < chunks)

    def before(clock):
        def fetch(u):
            c_arrival(u).wait_recv()
            c_load(u).start()

        u, on = turn(clock, 0)
        pl.when(inner & on)(functools.partial(fetch, u))

    def add_outer(u):
        @pl.when(u >= RING)
        def _():
            e_copy(u - RING).wait_send()

        _, i, r = place(u)
        c_load(u).wait()
        got = cload.at[lax.rem(u, 2)]
        xsend[lax.rem(u, RING)] = (part[i, r, pl.ds(other, hw)] + got[:, pl.ds(other, hw)].astype(F32)).astype(BF16)
        e_copy(u).start()
        part[i, r, pl.ds(mine, hw)] += got[:, pl.ds(mine, hw)].astype(F32)

    def add_across(u):
        @pl.when(u >= RING)
        def _():
            t_wait(u - RING)

        _, i, r = place(u)
        e_copy(u).wait_recv()
        tsend[lax.rem(u, RING)] = (part[i, r, pl.ds(mine, hw)] + xin[lax.rem(u, SLOTS)].astype(F32)).astype(BF16)
        for t in t_copies(u):
            t.start()

    def pass_outward(u):
        y_arrival(u, 0, other).wait_recv()
        for t in hand_on(u):
            t.start()

    def pass_across(u):
        near = pl.multiple_of(jnp.where(z == 3, hw, 0), hw)
        y_arrival(u, 0, near).wait_recv()
        y_arrival(u, 1, pl.multiple_of(hw - near, hw)).wait_recv()
        pass_over(u).start()

    def after(clock):
        for stage, (role, work) in enumerate(
            ((inner, add_outer), (inner, add_across), (inner, pass_outward), (outer, pass_across))
        ):
            u, on = turn(clock, stage)
            pl.when(role & on)(functools.partial(work, u))

    x_copy(0, BLOCK).start(priority=BULK)
    for t in a_copies(0, 0):
        t.start(priority=BULK)

    barrier = pltpu.get_barrier_semaphore()
    pl.semaphore_signal(barrier, inc=1, device_id=(dp, partner), device_id_type=MESH)

    @pl.when(inner)
    def _():
        pl.semaphore_signal(barrier, inc=1, device_id=(dp, outward), device_id_type=MESH)
        pl.semaphore_signal(barrier, inc=1, device_id=(dp, across), device_id_type=MESH)

    @pl.when(outer)
    def _():
        pl.semaphore_signal(barrier, inc=1, device_id=(dp, inward), device_id_type=MESH)

    def next_x(b):
        @pl.when(b + 1 < whole)
        def _():
            x_copy(b + 1, BLOCK).start(priority=BULK)

        if tail:
            @pl.when(b + 1 == whole)
            def _():
                x_copy(b + 1, tail).start(priority=BULK)

    def block(b, m, clock):
        x_copy(b, m).wait()
        mine_rows = pl.ds(0, m)

        @pl.when(b == 0)
        def _():
            for n in range(1, DEEP - 1):
                for t in a_copies(n, n):
                    t.start(priority=BULK)

        def a_step(n, clock):
            s, clock = lax.rem(n, DEEP), advance(clock, STEP_A)

            @pl.when(n + DEEP - 1 < steps_a)
            def _():
                for t in a_copies(n + DEEP - 1, lax.rem(n + DEEP - 1, DEEP)):
                    t.start(priority=BULK)

            @pl.when(n == steps_a - 1)
            def _():
                b_copy(par0, 0, 0).start(priority=BULK)
                b_copy(own0, 0, 1).start(priority=BULK)

            @pl.when((b == 0) & (n == steps_a - 1) & inner)
            def _():
                pl.semaphore_wait(barrier, 3)

            @pl.when((b == 0) & (n == steps_a - 1) & outer)
            def _():
                pl.semaphore_wait(barrier, 2)

            before(clock)
            for t in a_copies(n, s):
                t.wait()
            gate = jnp.dot(xb[mine_rows, :], wa[s, 0], preferred_element_type=F32)
            up = jnp.dot(xb[mine_rows, :], wa[s, 1], preferred_element_type=F32)
            hb[mine_rows, pl.ds(pl.multiple_of(n * NA, NA), NA)] = (jax.nn.silu(gate) * up).astype(BF16)
            after(clock)
            return clock

        clock = lax.fori_loop(0, steps_a, a_step, clock)
        next_x(b)

        def b_step(i, clock):
            clock, count = advance(clock, STEP_B), b * 4 + i
            b_copy(par0, i, 0).wait()

            @pl.when((count > 0) & (i > 0))
            def _():
                p_copy(m).wait_send()

            @pl.when((count > 0) & (i == 0))
            def _():
                p_copy(BLOCK).wait_send()

            before(clock)
            psend[mine_rows, :] = jnp.dot(hb[mine_rows, :], wb[0], preferred_element_type=F32).astype(BF16)

            @pl.when(count > 0)
            def _():
                pl.semaphore_wait(p_free, 1)

            p_copy(m).start()

            @pl.when(i < 3)
            def _():
                b_copy(par0, i + 1, 0).start(priority=BULK)

            @pl.when((i >= 5 - DEEP) & (b + 1 < blocks))
            def _():
                for t in a_copies(i - (5 - DEEP), i - (5 - DEEP)):
                    t.start(priority=BULK)

            after(clock)
            clock = advance(clock, STEP_B)
            before(clock)
            b_copy(own0, i, 1).wait()
            part[i, mine_rows, :] = jnp.dot(hb[mine_rows, :], wb[1], preferred_element_type=F32)

            @pl.when(i < 3)
            def _():
                b_copy(own0, i + 1, 1).start(priority=BULK)

            p_copy(m).wait_recv()

            @pl.when(inner)
            def _():
                part[i, mine_rows, :] += pbuf[mine_rows, :].astype(F32)

            @pl.when(outer)
            def _():
                @pl.when(b > 0)
                def _():
                    o_wait(i, BLOCK)

                for r in range(m // CHUNK):
                    at = pl.ds(r * CHUNK, CHUNK)
                    sent[i, at, :] = (part[i, at, :] + pbuf[at, :].astype(F32)).astype(BF16)
                    o_copy(b, i, r, b * 4 * per + i * (m // CHUNK) + r).start()

            @pl.when(count < blocks * 4 - 1)
            def _():
                pl.semaphore_signal(p_free, inc=1, device_id=(dp, partner), device_id_type=MESH)

            after(clock)
            return clock

        return lax.fori_loop(0, 4, b_step, clock)

    clock = (-steps_a * STEP_A, DUE) + (0,) * (max(LAGS) + 2)
    clock = lax.fori_loop(0, whole, lambda b, clock: block(b, BLOCK, clock), tuple(jnp.int32(v) for v in clock))
    if tail:
        clock = block(whole, tail, clock)

    def drain(_, clock):
        clock = advance(clock, tick)
        before(clock)
        after(clock)
        return clock

    left = chunks + max(BEHIND, max(LAGS)) - ((blocks - 1) * 4 * per + (8 * STEP_B - DUE) // tick)
    lax.fori_loop(0, left, drain, clock)

    p_copy(tail or BLOCK).wait_send()
    side = y.at[:, pl.ds(0, half)]
    quarter = y.at[:, pl.ds(0, half // 2)]

    @pl.when(outer)
    def _():
        for i in range(4):
            o_wait(i, tail or BLOCK)
        remote(side, side, g_send, yp_recv, partner).wait_send()

    @pl.when(inner)
    def _():
        for s in range(RING):
            e_copy(chunks - RING + s).wait_send()
            t_wait(chunks - RING + s)
        remote(quarter, quarter, f_send, yp_recv, partner).wait_send()
        remote(quarter, quarter, g_send, yp_recv, partner).wait_send()

    remote(side, side, g_send, yp_recv, partner).wait_recv()


def block_call(x, wg, wu, wd):
    rows, d = x.shape
    ff = wg.shape[1]
    half, nb = d // 2, d // 8
    hw = nb // 2
    chunks = rows // CHUNK * 4
    dma, any_ = pltpu.SemaphoreType.DMA, pl.BlockSpec(memory_space=pl.ANY)
    flops = 6 * rows * d * ff
    return pl.pallas_call(
        kernel,
        out_shape=[
            jax.ShapeDtypeStruct((rows, d), BF16),
            jax.ShapeDtypeStruct((rows, half), BF16),
        ],
        in_specs=[any_] * 4,
        out_specs=[any_] * 2,
        scratch_shapes=[
            pltpu.VMEM((BLOCK, d), BF16),
            pltpu.VMEM((BLOCK, ff), BF16),
            pltpu.VMEM((DEEP, 2, d, NA), BF16),
            pltpu.VMEM((2, ff, nb), BF16),
            pltpu.VMEM((4, BLOCK, nb), F32),
            pltpu.VMEM((4, BLOCK, nb), BF16),
            pltpu.VMEM((BLOCK, nb), BF16),
            pltpu.VMEM((BLOCK, nb), BF16),
            pltpu.VMEM((2, CHUNK, nb), BF16),
            pltpu.VMEM((SLOTS, CHUNK, hw), BF16),
            pltpu.VMEM((RING, CHUNK, hw), BF16),
            pltpu.VMEM((RING, CHUNK, hw), BF16),
            dma, dma((DEEP, 2)), dma((2,)), dma, dma, pltpu.SemaphoreType.REGULAR,
            dma((4,)), dma((chunks,)), dma((RING,)), dma((SLOTS,)),
            dma((RING, 4)), dma((2, chunks)), dma, dma, dma, dma((2,)),
        ],
        compiler_params=pltpu.CompilerParams(collective_id=0, has_side_effects=True, vmem_limit_bytes=VMEM),
        cost_estimate=pl.CostEstimate(flops=flops, bytes_accessed=10**9, transcendentals=rows * ff),
        name="mlp_block",
    )(x, wg, wu, wd)[0]


def solution(mesh):
    return jax.shard_map(
        block_call,
        mesh=mesh,
        in_specs=(P("dp", None), P(None, "tp"), P(None, "tp"), P("tp", None)),
        out_specs=P("dp", None),
        check_vma=False,
    )
```

```python
import functools

import jax
import jax.numpy as jnp
from jax import lax
from jax.experimental import pallas as pl
from jax.experimental.pallas import tpu as pltpu
from jax.sharding import PartitionSpec as P

MESH = pl.DeviceIdType.MESH
BF16, F32 = jnp.bfloat16, jnp.float32
BLOCK, CHUNK, NA = 384, 128, 256
BULK = 1
FIRST, COPY_FLOPS = 11, 10**9
LATE = 2
VMEM = 67043328
SLOTS, RING, DEEP = 8, 4, 3
STEP_A, STEP_B, DUE, TICK = 184, 144, 700, 270
TAIL_A, TAIL_B = 130, 94
LAGS, BEHIND = (0, 2, 5), 16


def kernel(
    x, wg, wu, wd,
    y, cin, late,
    xb, hb, wa, wb, part, sent, psend, pbuf, cload, xin, xsend, tsend,
    sx, sa, sb, p_send, p_recv, p_free, o_send, c_recv, x_send, x_recv,
    t_send, y_recv, f_send, g_send, yp_recv, l_sem,
):
    rows, d = x.shape
    ff = wg.shape[1]
    half, nb = d // 2, d // 8
    hw = nb // 2
    steps_a, whole, per = ff // NA, rows // BLOCK, BLOCK // CHUNK
    tail = rows - whole * BLOCK
    blocks, chunks, per_tail = whole + (tail > 0), rows // CHUNK * 4, max(tail // CHUNK, 1)
    tick = TICK

    dp, me = lax.axis_index("dp"), lax.axis_index("tp")
    z, c = me // 2, me % 2
    inner = (z == 1) | (z == 2)
    outer = jnp.logical_not(inner)
    partner = me + 1 - 2 * c
    inward = (1 + z // 2) * 2 + c
    outward = (3 * (z - 1)) * 2 + c
    across = (3 - z) * 2 + c
    mine = pl.multiple_of(jnp.where(z == 2, hw, 0), hw)
    other = pl.multiple_of(hw - mine, hw)
    near = pl.multiple_of(jnp.where(z == 3, hw, 0), hw)
    own0, par0 = c * half, (1 - c) * half

    def remote(src, dst, send, recv, to):
        return pltpu.make_async_remote_copy(
            src_ref=src, dst_ref=dst, send_sem=send, recv_sem=recv,
            device_id=(dp, to), device_id_type=MESH,
        )

    def place(u):
        b, w = lax.div(u, 4 * per), lax.rem(u, 4 * per)
        n = jnp.where(b < whole, per, per_tail)
        i = jnp.where(b < whole, lax.div(w, per), lax.div(w, per_tail))
        r = w - i * n
        return (
            pl.ds(pl.multiple_of(b * BLOCK + r * CHUNK, CHUNK), CHUNK), i, pl.ds(pl.multiple_of(r * CHUNK, CHUNK), CHUNK)
        )

    def cols(base, i, off, n):
        return pl.ds(pl.multiple_of(base + i * nb + off, n), n)

    def x_copy(b, m):
        return pltpu.make_async_copy(x.at[pl.ds(pl.multiple_of(b * BLOCK, CHUNK), m), :], xb.at[pl.ds(0, m), :], sx)

    def a_copies(n, s):
        col = pl.ds(pl.multiple_of(n * NA, NA), NA)
        return [pltpu.make_async_copy(w.at[:, col], wa.at[s, j], sa.at[s, j]) for j, w in enumerate((wg, wu))]

    def b_copy(base, i, s):
        return pltpu.make_async_copy(wd.at[:, cols(base, i, 0, nb)], wb.at[s], sb.at[s])

    def p_copy(m):
        return remote(psend.at[pl.ds(0, m), :], pbuf.at[pl.ds(0, m), :], p_send, p_recv, partner)

    def o_copies(b, i, r, u):
        rw = pl.ds(pl.multiple_of(b * BLOCK + r * CHUNK, CHUNK), CHUNK)
        return [
            remote(
                sent.at[i, pl.ds(r * CHUNK, CHUNK), pl.ds(off, hw)], cin.at[rw, cols(0, i, off, hw)],
                o_send.at[i], c_recv.at[j, u], inward,
            )
            for j, off in enumerate((pl.multiple_of(hw - near, hw), near))
        ]

    def o_wait(i, m):
        at = pl.ds(0, m)
        remote(sent.at[i, at, :], cin.at[at, cols(0, i, 0, nb)], o_send.at[i], c_recv.at[0, 0], inward).wait_send()

    def c_half(u, j):
        rw, i, _ = place(u)
        return cin.at[rw, cols(0, i, (other, mine)[j], hw)]

    def c_arrival(u, j):
        return remote(c_half(u, j), c_half(u, j), o_send.at[0], c_recv.at[j, u], outward)

    def c_load(u, j):
        s = lax.rem(u, 2)
        return pltpu.make_async_copy(c_half(u, j), cload.at[j, s], l_sem.at[j, s])

    def e_copy(u):
        return remote(xsend.at[lax.rem(u, RING)], xin.at[lax.rem(u, SLOTS)], x_send.at[lax.rem(u, RING)], x_recv.at[lax.rem(u, SLOTS)], across)

    def t_copies(u):
        rw, i, _ = place(u)
        dst, s = y.at[rw, cols(own0, i, mine, hw)], lax.rem(u, RING)
        src = tsend.at[s]
        return [
            remote(src, dst, t_send.at[s, 0], y_recv.at[0, u], outward),
            remote(src, dst, t_send.at[s, 1], y_recv.at[0, u], across),
            remote(src, dst, t_send.at[s, 2], yp_recv, partner),
            pltpu.make_async_copy(src, dst, t_send.at[s, 3]),
        ]

    def t_wait(u):
        near_copy, *others, here = t_copies(u)
        pl.when(u < chunks - LATE)(near_copy.wait_send)
        for t in others:
            t.wait_send()
        here.wait()

    def hand_on(u):
        rw, i, _ = place(u)
        at = y.at[rw, cols(own0, i, other, hw)]
        return remote(at, at, f_send, y_recv.at[1, u], outward), remote(at, at, g_send, yp_recv, partner)

    def pass_over(u):
        rw, i, _ = place(u)
        at = y.at[rw, cols(own0, i, 0, nb)]
        return remote(at, at, g_send, yp_recv, partner)

    def y_arrival(u, kind, off):
        rw, i, _ = place(u)
        at = y.at[rw, cols(own0, i, off, hw)]
        return remote(at, at, f_send, y_recv.at[kind, u], across)

    def advance(clock, step):
        t, due, *made = clock
        t = t + step
        on = jnp.where(t >= due, 1, 0)
        return (t, due + tick * on, made[0] + on, *made[:-1])

    def turn(clock, stage):
        made = clock[2:]
        lag, behind = (LAGS[stage], 0) if stage < 3 else (0, BEHIND)
        u = made[lag + 1] - behind
        return u, (made[lag] > made[lag + 1]) & (u >= 0) & (u < chunks - LATE * (stage == 3))

    def before(clock):
        def fetch(u, j):
            c_arrival(u, j).wait_recv()
            c_load(u, j).start()

        for j in (0, 1):
            u, on = turn(clock, j)
            pl.when(inner & on)(functools.partial(fetch, u, j))

    def add_outer(u):
        @pl.when(u >= RING)
        def _():
            e_copy(u - RING).wait_send()

        _, i, r = place(u)
        c_load(u, 0).wait()
        xsend[lax.rem(u, RING)] = (part[i, r, pl.ds(other, hw)] + cload[0, lax.rem(u, 2)].astype(F32)).astype(BF16)
        e_copy(u).start()

    def add_across(u):
        @pl.when(u >= RING)
        def _():
            t_wait(u - RING)

        _, i, r = place(u)
        c_load(u, 1).wait()
        here = part[i, r, pl.ds(mine, hw)] + cload[1, lax.rem(u, 2)].astype(F32)
        e_copy(u).wait_recv()
        tsend[lax.rem(u, RING)] = (here + xin[lax.rem(u, SLOTS)].astype(F32)).astype(BF16)
        near_copy, *others = t_copies(u)
        pl.when(u < chunks - LATE)(near_copy.start)
        for t in others:
            t.start()

    def pass_outward(u):
        y_arrival(u, 0, other).wait_recv()
        out, over = hand_on(u)
        pl.when(u < chunks - LATE)(out.start)
        over.start()

    def pass_across(u):
        y_arrival(u, 0, near).wait_recv()
        y_arrival(u, 1, pl.multiple_of(hw - near, hw)).wait_recv()
        pass_over(u).start()

    def after(clock):
        for stage, (role, work) in enumerate(
            ((inner, add_outer), (inner, add_across), (inner, pass_outward), (outer, pass_across))
        ):
            u, on = turn(clock, stage)
            pl.when(role & on)(functools.partial(work, u))

    x_copy(0, BLOCK).start(priority=BULK)
    for t in a_copies(0, 0):
        t.start(priority=BULK)

    barrier = pltpu.get_barrier_semaphore()
    pl.semaphore_signal(barrier, inc=1, device_id=(dp, partner), device_id_type=MESH)

    @pl.when(inner)
    def _():
        pl.semaphore_signal(barrier, inc=1, device_id=(dp, outward), device_id_type=MESH)
        pl.semaphore_signal(barrier, inc=1, device_id=(dp, across), device_id_type=MESH)

    @pl.when(outer)
    def _():
        pl.semaphore_signal(barrier, inc=1, device_id=(dp, inward), device_id_type=MESH)

    def next_x(b):
        @pl.when(b + 1 < whole)
        def _():
            x_copy(b + 1, BLOCK).start(priority=BULK)

        if tail:
            @pl.when(b + 1 == whole)
            def _():
                x_copy(b + 1, tail).start(priority=BULK)

    def block(b, m, clock, long_a, long_b):
        x_copy(b, m).wait()
        mine_rows = pl.ds(0, m)

        @pl.when(b == 0)
        def _():
            for n in range(1, DEEP - 1):
                for t in a_copies(n, n):
                    t.start(priority=BULK)

        def a_step(n, clock):
            s, clock = lax.rem(n, DEEP), advance(clock, long_a)

            @pl.when(n + DEEP - 1 < steps_a)
            def _():
                for t in a_copies(n + DEEP - 1, lax.rem(n + DEEP - 1, DEEP)):
                    t.start(priority=BULK)

            @pl.when(n == steps_a - 1)
            def _():
                b_copy(par0, 0, 0).start(priority=BULK)
                b_copy(own0, 0, 1).start(priority=BULK)

            @pl.when((b == 0) & (n == steps_a - 1) & inner)
            def _():
                pl.semaphore_wait(barrier, 3)

            @pl.when((b == 0) & (n == steps_a - 1) & outer)
            def _():
                pl.semaphore_wait(barrier, 2)

            before(clock)
            for t in a_copies(n, s):
                t.wait()
            gate = jnp.dot(xb[mine_rows, :], wa[s, 0], preferred_element_type=F32)
            up = jnp.dot(xb[mine_rows, :], wa[s, 1], preferred_element_type=F32)
            hb[mine_rows, pl.ds(pl.multiple_of(n * NA, NA), NA)] = (jax.nn.silu(gate) * up).astype(BF16)
            after(clock)
            return clock

        clock = lax.fori_loop(0, steps_a, a_step, clock)
        next_x(b)

        def b_step(i, clock):
            clock, count = advance(clock, long_b), b * 4 + i
            b_copy(par0, i, 0).wait()

            @pl.when((count > 0) & (i > 0))
            def _():
                p_copy(m).wait_send()

            @pl.when((count > 0) & (i == 0))
            def _():
                p_copy(BLOCK).wait_send()

            before(clock)
            psend[mine_rows, :] = jnp.dot(hb[mine_rows, :], wb[0], preferred_element_type=F32).astype(BF16)

            @pl.when(count > 0)
            def _():
                pl.semaphore_wait(p_free, 1)

            p_copy(m).start()

            @pl.when(i < 3)
            def _():
                b_copy(par0, i + 1, 0).start(priority=BULK)

            @pl.when((i >= 5 - DEEP) & (b + 1 < blocks))
            def _():
                for t in a_copies(i - (5 - DEEP), i - (5 - DEEP)):
                    t.start(priority=BULK)

            after(clock)
            clock = advance(clock, long_b)
            before(clock)
            b_copy(own0, i, 1).wait()
            part[i, mine_rows, :] = jnp.dot(hb[mine_rows, :], wb[1], preferred_element_type=F32)

            @pl.when(i < 3)
            def _():
                b_copy(own0, i + 1, 1).start(priority=BULK)

            p_copy(m).wait_recv()

            @pl.when(inner)
            def _():
                part[i, mine_rows, :] += pbuf[mine_rows, :].astype(F32)

            @pl.when(outer)
            def _():
                @pl.when(b > 0)
                def _():
                    o_wait(i, BLOCK)

                for r in range(m // CHUNK):
                    at = pl.ds(r * CHUNK, CHUNK)
                    sent[i, at, :] = (part[i, at, :] + pbuf[at, :].astype(F32)).astype(BF16)
                    for o in o_copies(b, i, r, b * 4 * per + i * (m // CHUNK) + r):
                        o.start()

            @pl.when(count < blocks * 4 - 1)
            def _():
                pl.semaphore_signal(p_free, inc=1, device_id=(dp, partner), device_id_type=MESH)

            after(clock)
            return clock

        return lax.fori_loop(0, 4, b_step, clock)

    clock = (-steps_a * STEP_A, DUE) + (0,) * (max(LAGS) + 2)
    clock = lax.fori_loop(0, whole, lambda b, clock: block(b, BLOCK, clock, STEP_A, STEP_B), tuple(jnp.int32(v) for v in clock))
    if tail:
        clock = block(whole, tail, clock, TAIL_A, TAIL_B)

    def drain(_, clock):
        clock = advance(clock, tick)
        before(clock)
        after(clock)
        return clock

    end = (whole - 1) * (steps_a * STEP_A + 8 * STEP_B) + 8 * STEP_B + (tail > 0) * (steps_a * TAIL_A + 8 * TAIL_B)
    left = chunks + max(BEHIND, max(LAGS)) - (end - DUE) // tick
    lax.fori_loop(0, left, drain, clock)

    p_copy(tail or BLOCK).wait_send()

    def bytes_of(count, columns):
        return y.at[pl.ds(0, count * CHUNK * columns // d), :]

    early = chunks - LATE

    @pl.when(outer)
    def _():
        for i in range(4):
            o_wait(i, tail or BLOCK)
        passed = bytes_of(early, nb)
        remote(passed, passed, g_send, yp_recv, partner).wait_send()
        remote(passed, passed, g_send, yp_recv, partner).wait_recv()

    @pl.when(inner)
    def _():
        for s in range(RING):
            e_copy(chunks - RING + s).wait_send()
            t_wait(chunks - RING + s)
        out, over, took = bytes_of(early, hw), bytes_of(chunks, hw), bytes_of(chunks, nb)
        remote(out, out, f_send, yp_recv, partner).wait_send()
        remote(over, over, g_send, yp_recv, partner).wait_send()
        remote(took, took, g_send, yp_recv, partner).wait_recv()
        moves = []
        for s in range(late.shape[1] // hw):
            src = y.at[pl.ds(rows - CHUNK, CHUNK), pl.ds(pl.multiple_of(own0 + half - late.shape[1] + s * hw, hw), hw)]
            moves.append((
                pltpu.make_async_copy(src, tsend.at[s], t_send.at[s, 0]),
                pltpu.make_async_copy(tsend.at[s], late.at[:, pl.ds(s * hw, hw)], t_send.at[s, 1]),
            ))
        for read, _ in moves:
            read.start()
        for read, write in moves:
            read.wait()
            write.start()
        for _, write in moves:
            write.wait()


def copy_rows(first, count, src, *refs):
    dst, held, read, written = refs[-4:]

    def move(k):
        rows = pl.ds((first + k) * CHUNK, CHUNK)
        return (
            pltpu.make_async_copy(src.at[rows, :], held.at[k], read.at[k]),
            pltpu.make_async_copy(held.at[k], dst.at[rows, :], written.at[k]),
        )

    for k in range(count):
        move(k)[0].start()
    for k in range(count):
        move(k)[0].wait()
        move(k)[1].start()
    for k in range(count):
        move(k)[1].wait()


def add_late(y_in, own, par, y, held, read, written):
    rows, d = y.shape
    me = lax.axis_index("tp")
    z, c = me // 2, me % 2
    wide = own.shape[1]

    @pl.when((z == 0) | (z == 3))
    def _():
        moves = []
        for j, (src, side) in enumerate(((own, c), (par, 1 - c))):
            to = y.at[pl.ds(rows - CHUNK, CHUNK), pl.ds(pl.multiple_of(side * (d // 2) + d // 2 - wide, wide), wide)]
            moves.append((
                pltpu.make_async_copy(src, held.at[j], read.at[j]),
                pltpu.make_async_copy(held.at[j], to, written.at[j]),
            ))
        for r, _ in moves:
            r.start()
        for r, w in moves:
            r.wait()
            w.start()
        for _, w in moves:
            w.wait()


def block_call(x, wg, wu, wd):
    rows, d = x.shape
    ff = wg.shape[1]
    half, nb = d // 2, d // 8
    hw = nb // 2
    chunks = rows // CHUNK * 4
    dma, any_ = pltpu.SemaphoreType.DMA, pl.BlockSpec(memory_space=pl.ANY)
    flops = 6 * rows * d * ff
    summed, _, late = pl.pallas_call(
        kernel,
        out_shape=[
            jax.ShapeDtypeStruct((rows, d), BF16),
            jax.ShapeDtypeStruct((rows, half), BF16),
            jax.ShapeDtypeStruct((CHUNK, LATE * nb), BF16),
        ],
        in_specs=[any_] * 4,
        out_specs=[any_] * 3,
        scratch_shapes=[
            pltpu.VMEM((BLOCK, d), BF16),
            pltpu.VMEM((BLOCK, ff), BF16),
            pltpu.VMEM((DEEP, 2, d, NA), BF16),
            pltpu.VMEM((2, ff, nb), BF16),
            pltpu.VMEM((4, BLOCK, nb), F32),
            pltpu.VMEM((4, BLOCK, nb), BF16),
            pltpu.VMEM((BLOCK, nb), BF16),
            pltpu.VMEM((BLOCK, nb), BF16),
            pltpu.VMEM((2, 2, CHUNK, hw), BF16),
            pltpu.VMEM((SLOTS, CHUNK, hw), BF16),
            pltpu.VMEM((RING, CHUNK, hw), BF16),
            pltpu.VMEM((RING, CHUNK, hw), BF16),
            dma, dma((DEEP, 2)), dma((2,)), dma, dma, pltpu.SemaphoreType.REGULAR,
            dma((4,)), dma((2, chunks)), dma((RING,)), dma((SLOTS,)),
            dma((RING, 4)), dma((2, chunks)), dma, dma, dma, dma((2, 2)),
        ],
        compiler_params=pltpu.CompilerParams(collective_id=0, has_side_effects=True, vmem_limit_bytes=VMEM),
        cost_estimate=pl.CostEstimate(flops=flops, bytes_accessed=10**9, transcendentals=rows * ff),
        name="mlp_block",
    )(x, wg, wu, wd)

    wide = LATE * nb
    own = lax.ppermute(late, "tp", [(2, 0), (3, 1), (4, 6), (5, 7)])
    out = jax.ShapeDtypeStruct((rows, d), BF16)
    params = pltpu.CompilerParams(vmem_limit_bytes=VMEM)

    def copy_call(first, count, extra, alias, name):
        return pl.pallas_call(
            functools.partial(copy_rows, first, count),
            out_shape=out,
            in_specs=[any_] * (1 + len(extra)),
            out_specs=any_,
            scratch_shapes=[pltpu.VMEM((count, CHUNK, d), BF16), dma((count,)), dma((count,))],
            input_output_aliases=alias,
            compiler_params=params,
            cost_estimate=pl.CostEstimate(flops=count * COPY_FLOPS, bytes_accessed=count * CHUNK * d * 4, transcendentals=0),
            name=name,
        )(summed, *extra)

    own, y = lax.optimization_barrier((own, copy_call(0, FIRST, (), {}, "copy_first")))
    par = lax.ppermute(own, "tp", [(0, 1), (1, 0), (6, 7), (7, 6)])
    y = copy_call(FIRST, rows // CHUNK - FIRST, (own, y), {2: 0}, "copy_rest")
    return pl.pallas_call(
        add_late,
        out_shape=out,
        in_specs=[any_] * 3,
        out_specs=any_,
        scratch_shapes=[pltpu.VMEM((2, CHUNK, wide), BF16), dma((2,)), dma((2,))],
        input_output_aliases={0: 0},
        compiler_params=params,
        name="late_chunks",
    )(y, own, par)


def solution(mesh):
    return jax.shard_map(
        block_call,
        mesh=mesh,
        in_specs=(P("dp", None), P(None, "tp"), P(None, "tp"), P("tp", None)),
        out_specs=P("dp", None),
        check_vma=False,
    )
```

```python
import functools

import jax
import jax.numpy as jnp
from jax import lax
from jax.experimental import pallas as pl
from jax.experimental.pallas import tpu as pltpu
from jax.sharding import PartitionSpec as P

MESH = pl.DeviceIdType.MESH
BF16, F32 = jnp.bfloat16, jnp.float32
BLOCK, CHUNK, NA = 384, 128, 256
BULK = 1
PIECE, FIRST, COPY_FLOPS = 32, 44, 25 * 10**7
LATE = 2
VMEM = 67043328
SLOTS, RING, DEEP = 8, 4, 3
STEP_A, STEP_B, DUE, TICK = 184, 144, 700, 270
TAIL_A, TAIL_B = 130, 94
LAGS, BEHIND = (0, 2, 5), 16


def kernel(
    x, wg, wu, wd,
    y, cin, late,
    xb, hb, wa, wb, part, sent, psend, pbuf, cload, xin, xsend, tsend,
    sx, sa, sb, p_send, p_recv, p_free, o_send, c_recv, x_send, x_recv,
    t_send, y_recv, f_send, g_send, yp_recv, l_sem,
):
    rows, d = x.shape
    ff = wg.shape[1]
    half, nb = d // 2, d // 8
    hw = nb // 2
    steps_a, whole, per = ff // NA, rows // BLOCK, BLOCK // CHUNK
    tail = rows - whole * BLOCK
    blocks, chunks, per_tail = whole + (tail > 0), rows // CHUNK * 4, max(tail // CHUNK, 1)
    tick = TICK

    dp, me = lax.axis_index("dp"), lax.axis_index("tp")
    z, c = me // 2, me % 2
    inner = (z == 1) | (z == 2)
    outer = jnp.logical_not(inner)
    partner = me + 1 - 2 * c
    inward = (1 + z // 2) * 2 + c
    outward = (3 * (z - 1)) * 2 + c
    across = (3 - z) * 2 + c
    mine = pl.multiple_of(jnp.where(z == 2, hw, 0), hw)
    other = pl.multiple_of(hw - mine, hw)
    near = pl.multiple_of(jnp.where(z == 3, hw, 0), hw)
    own0, par0 = c * half, (1 - c) * half

    def remote(src, dst, send, recv, to):
        return pltpu.make_async_remote_copy(
            src_ref=src, dst_ref=dst, send_sem=send, recv_sem=recv,
            device_id=(dp, to), device_id_type=MESH,
        )

    def place(u):
        b, w = lax.div(u, 4 * per), lax.rem(u, 4 * per)
        n = jnp.where(b < whole, per, per_tail)
        i = jnp.where(b < whole, lax.div(w, per), lax.div(w, per_tail))
        r = w - i * n
        return (
            pl.ds(pl.multiple_of(b * BLOCK + r * CHUNK, CHUNK), CHUNK), i, pl.ds(pl.multiple_of(r * CHUNK, CHUNK), CHUNK)
        )

    def cols(base, i, off, n):
        return pl.ds(pl.multiple_of(base + i * nb + off, n), n)

    def x_copy(b, m):
        return pltpu.make_async_copy(x.at[pl.ds(pl.multiple_of(b * BLOCK, CHUNK), m), :], xb.at[pl.ds(0, m), :], sx)

    def a_copies(n, s):
        col = pl.ds(pl.multiple_of(n * NA, NA), NA)
        return [pltpu.make_async_copy(w.at[:, col], wa.at[s, j], sa.at[s, j]) for j, w in enumerate((wg, wu))]

    def b_copy(base, i, s):
        return pltpu.make_async_copy(wd.at[:, cols(base, i, 0, nb)], wb.at[s], sb.at[s])

    def p_copy(m):
        return remote(psend.at[pl.ds(0, m), :], pbuf.at[pl.ds(0, m), :], p_send, p_recv, partner)

    def o_copies(b, i, r, u):
        rw = pl.ds(pl.multiple_of(b * BLOCK + r * CHUNK, CHUNK), CHUNK)
        return [
            remote(
                sent.at[i, pl.ds(r * CHUNK, CHUNK), pl.ds(off, hw)], cin.at[rw, cols(0, i, off, hw)],
                o_send.at[i], c_recv.at[j, u], inward,
            )
            for j, off in enumerate((pl.multiple_of(hw - near, hw), near))
        ]

    def o_wait(i, m):
        at = pl.ds(0, m)
        remote(sent.at[i, at, :], cin.at[at, cols(0, i, 0, nb)], o_send.at[i], c_recv.at[0, 0], inward).wait_send()

    def c_half(u, j):
        rw, i, _ = place(u)
        return cin.at[rw, cols(0, i, (other, mine)[j], hw)]

    def c_arrival(u, j):
        return remote(c_half(u, j), c_half(u, j), o_send.at[0], c_recv.at[j, u], outward)

    def c_load(u, j):
        s = lax.rem(u, 2)
        return pltpu.make_async_copy(c_half(u, j), cload.at[j, s], l_sem.at[j, s])

    def e_copy(u):
        return remote(xsend.at[lax.rem(u, RING)], xin.at[lax.rem(u, SLOTS)], x_send.at[lax.rem(u, RING)], x_recv.at[lax.rem(u, SLOTS)], across)

    def t_copies(u):
        rw, i, _ = place(u)
        dst, s = y.at[rw, cols(own0, i, mine, hw)], lax.rem(u, RING)
        src = tsend.at[s]
        return [
            remote(src, dst, t_send.at[s, 0], y_recv.at[0, u], outward),
            remote(src, dst, t_send.at[s, 1], y_recv.at[0, u], across),
            remote(src, dst, t_send.at[s, 2], yp_recv, partner),
            pltpu.make_async_copy(src, dst, t_send.at[s, 3]),
        ]

    def t_wait(u):
        near_copy, *others, here = t_copies(u)
        pl.when(u < chunks - LATE)(near_copy.wait_send)
        for t in others:
            t.wait_send()
        here.wait()

    def hand_on(u):
        rw, i, _ = place(u)
        at = y.at[rw, cols(own0, i, other, hw)]
        return remote(at, at, f_send, y_recv.at[1, u], outward), remote(at, at, g_send, yp_recv, partner)

    def pass_over(u):
        rw, i, _ = place(u)
        at = y.at[rw, cols(own0, i, 0, nb)]
        return remote(at, at, g_send, yp_recv, partner)

    def y_arrival(u, kind, off):
        rw, i, _ = place(u)
        at = y.at[rw, cols(own0, i, off, hw)]
        return remote(at, at, f_send, y_recv.at[kind, u], across)

    def advance(clock, step):
        t, due, *made = clock
        t = t + step
        on = jnp.where(t >= due, 1, 0)
        return (t, due + tick * on, made[0] + on, *made[:-1])

    def turn(clock, stage):
        made = clock[2:]
        lag, behind = (LAGS[stage], 0) if stage < 3 else (0, BEHIND)
        u = made[lag + 1] - behind
        return u, (made[lag] > made[lag + 1]) & (u >= 0) & (u < chunks - LATE * (stage == 3))

    def before(clock):
        def fetch(u, j):
            c_arrival(u, j).wait_recv()
            c_load(u, j).start()

        for j in (0, 1):
            u, on = turn(clock, j)
            pl.when(inner & on)(functools.partial(fetch, u, j))

    def add_outer(u):
        @pl.when(u >= RING)
        def _():
            e_copy(u - RING).wait_send()

        _, i, r = place(u)
        c_load(u, 0).wait()
        xsend[lax.rem(u, RING)] = (part[i, r, pl.ds(other, hw)] + cload[0, lax.rem(u, 2)].astype(F32)).astype(BF16)
        e_copy(u).start()

    def add_across(u):
        @pl.when(u >= RING)
        def _():
            t_wait(u - RING)

        _, i, r = place(u)
        c_load(u, 1).wait()
        here = part[i, r, pl.ds(mine, hw)] + cload[1, lax.rem(u, 2)].astype(F32)
        e_copy(u).wait_recv()
        tsend[lax.rem(u, RING)] = (here + xin[lax.rem(u, SLOTS)].astype(F32)).astype(BF16)
        near_copy, *others = t_copies(u)
        pl.when(u < chunks - LATE)(near_copy.start)
        for t in others:
            t.start()

    def pass_outward(u):
        y_arrival(u, 0, other).wait_recv()
        out, over = hand_on(u)
        pl.when(u < chunks - LATE)(out.start)
        over.start()

    def pass_across(u):
        y_arrival(u, 0, near).wait_recv()
        y_arrival(u, 1, pl.multiple_of(hw - near, hw)).wait_recv()
        pass_over(u).start()

    def after(clock):
        for stage, (role, work) in enumerate(
            ((inner, add_outer), (inner, add_across), (inner, pass_outward), (outer, pass_across))
        ):
            u, on = turn(clock, stage)
            pl.when(role & on)(functools.partial(work, u))

    x_copy(0, BLOCK).start(priority=BULK)
    for t in a_copies(0, 0):
        t.start(priority=BULK)

    barrier = pltpu.get_barrier_semaphore()
    pl.semaphore_signal(barrier, inc=1, device_id=(dp, partner), device_id_type=MESH)

    @pl.when(inner)
    def _():
        pl.semaphore_signal(barrier, inc=1, device_id=(dp, outward), device_id_type=MESH)
        pl.semaphore_signal(barrier, inc=1, device_id=(dp, across), device_id_type=MESH)

    @pl.when(outer)
    def _():
        pl.semaphore_signal(barrier, inc=1, device_id=(dp, inward), device_id_type=MESH)

    def next_x(b):
        @pl.when(b + 1 < whole)
        def _():
            x_copy(b + 1, BLOCK).start(priority=BULK)

        if tail:
            @pl.when(b + 1 == whole)
            def _():
                x_copy(b + 1, tail).start(priority=BULK)

    def block(b, m, clock, long_a, long_b):
        x_copy(b, m).wait()
        mine_rows = pl.ds(0, m)

        for n in range(1, DEEP - 1):
            for t in a_copies(n, n):
                t.start(priority=BULK)

        def a_step(n, clock):
            s, clock = lax.rem(n, DEEP), advance(clock, long_a)

            @pl.when(n + DEEP - 1 < steps_a)
            def _():
                for t in a_copies(n + DEEP - 1, lax.rem(n + DEEP - 1, DEEP)):
                    t.start(priority=BULK)

            @pl.when(n == steps_a - 1)
            def _():
                b_copy(par0, 0, 0).start(priority=BULK)
                b_copy(own0, 0, 1).start(priority=BULK)

            @pl.when((b == 0) & (n == steps_a - 1) & inner)
            def _():
                pl.semaphore_wait(barrier, 3)

            @pl.when((b == 0) & (n == steps_a - 1) & outer)
            def _():
                pl.semaphore_wait(barrier, 2)

            before(clock)
            for t in a_copies(n, s):
                t.wait()
            gate = jnp.dot(xb[mine_rows, :], wa[s, 0], preferred_element_type=F32)
            up = jnp.dot(xb[mine_rows, :], wa[s, 1], preferred_element_type=F32)
            hb[mine_rows, pl.ds(pl.multiple_of(n * NA, NA), NA)] = (jax.nn.silu(gate) * up).astype(BF16)
            after(clock)
            return clock

        clock = lax.fori_loop(0, steps_a, a_step, clock)
        next_x(b)

        def b_step(i, clock):
            clock, count = advance(clock, long_b), b * 4 + i
            b_copy(par0, i, 0).wait()

            @pl.when((count > 0) & (i > 0))
            def _():
                p_copy(m).wait_send()

            @pl.when((count > 0) & (i == 0))
            def _():
                p_copy(BLOCK).wait_send()

            before(clock)
            psend[mine_rows, :] = jnp.dot(hb[mine_rows, :], wb[0], preferred_element_type=F32).astype(BF16)

            @pl.when(count > 0)
            def _():
                pl.semaphore_wait(p_free, 1)

            p_copy(m).start()

            @pl.when(i < 3)
            def _():
                b_copy(par0, i + 1, 0).start(priority=BULK)

            @pl.when((i == 3) & (b + 1 < blocks))
            def _():
                for t in a_copies(0, 0):
                    t.start(priority=BULK)

            after(clock)
            clock = advance(clock, long_b)
            before(clock)
            b_copy(own0, i, 1).wait()
            part[i, mine_rows, :] = jnp.dot(hb[mine_rows, :], wb[1], preferred_element_type=F32)

            @pl.when(i < 3)
            def _():
                b_copy(own0, i + 1, 1).start(priority=BULK)

            p_copy(m).wait_recv()

            @pl.when(inner)
            def _():
                part[i, mine_rows, :] += pbuf[mine_rows, :].astype(F32)

            @pl.when(outer)
            def _():
                @pl.when(b > 0)
                def _():
                    o_wait(i, BLOCK)

                for r in range(m // CHUNK):
                    at = pl.ds(r * CHUNK, CHUNK)
                    sent[i, at, :] = (part[i, at, :] + pbuf[at, :].astype(F32)).astype(BF16)
                    for o in o_copies(b, i, r, b * 4 * per + i * (m // CHUNK) + r):
                        o.start()

            @pl.when(count < blocks * 4 - 1)
            def _():
                pl.semaphore_signal(p_free, inc=1, device_id=(dp, partner), device_id_type=MESH)

            after(clock)
            return clock

        return lax.fori_loop(0, 4, b_step, clock)

    clock = (-steps_a * STEP_A, DUE) + (0,) * (max(LAGS) + 2)
    clock = lax.fori_loop(0, whole, lambda b, clock: block(b, BLOCK, clock, STEP_A, STEP_B), tuple(jnp.int32(v) for v in clock))
    if tail:
        clock = block(whole, tail, clock, TAIL_A, TAIL_B)

    def drain(_, clock):
        clock = advance(clock, tick)
        before(clock)
        after(clock)
        return clock

    end = (whole - 1) * (steps_a * STEP_A + 8 * STEP_B) + 8 * STEP_B + (tail > 0) * (steps_a * TAIL_A + 8 * TAIL_B)
    left = chunks + max(BEHIND, max(LAGS)) - (end - DUE) // tick
    lax.fori_loop(0, left, drain, clock)

    p_copy(tail or BLOCK).wait_send()

    def bytes_of(count, columns):
        return y.at[pl.ds(0, count * CHUNK * columns // d), :]

    early = chunks - LATE

    @pl.when(outer)
    def _():
        for i in range(4):
            o_wait(i, tail or BLOCK)
        passed = bytes_of(early, nb)
        remote(passed, passed, g_send, yp_recv, partner).wait_send()
        remote(passed, passed, g_send, yp_recv, partner).wait_recv()

    @pl.when(inner)
    def _():
        for s in range(RING):
            e_copy(chunks - RING + s).wait_send()
            t_wait(chunks - RING + s)
        out, over, took = bytes_of(early, hw), bytes_of(chunks, hw), bytes_of(chunks, nb)
        remote(out, out, f_send, yp_recv, partner).wait_send()
        remote(over, over, g_send, yp_recv, partner).wait_send()
        remote(took, took, g_send, yp_recv, partner).wait_recv()
        moves = []
        for s in range(late.shape[1] // hw):
            src = y.at[pl.ds(rows - CHUNK, CHUNK), pl.ds(pl.multiple_of(own0 + half - late.shape[1] + s * hw, hw), hw)]
            moves.append((
                pltpu.make_async_copy(src, tsend.at[s], t_send.at[s, 0]),
                pltpu.make_async_copy(tsend.at[s], late.at[:, pl.ds(s * hw, hw)], t_send.at[s, 1]),
            ))
        for read, _ in moves:
            read.start()
        for read, write in moves:
            read.wait()
            write.start()
        for _, write in moves:
            write.wait()


def copy_rows(first, count, src, *refs):
    dst, held, read, written = refs[-4:]

    def move(k):
        rows = pl.ds((first + k) * PIECE, PIECE)
        return (
            pltpu.make_async_copy(src.at[rows, :], held.at[k], read.at[k]),
            pltpu.make_async_copy(held.at[k], dst.at[rows, :], written.at[k]),
        )

    for k in range(count):
        move(k)[0].start()
    for k in range(count):
        move(k)[0].wait()
        move(k)[1].start()
    for k in range(count):
        move(k)[1].wait()


def add_late(y_in, own, par, y, held, read, written):
    rows, d = y.shape
    me = lax.axis_index("tp")
    z, c = me // 2, me % 2
    wide = own.shape[1]

    @pl.when((z == 0) | (z == 3))
    def _():
        moves = []
        for j, (src, side) in enumerate(((own, c), (par, 1 - c))):
            to = y.at[pl.ds(rows - CHUNK, CHUNK), pl.ds(pl.multiple_of(side * (d // 2) + d // 2 - wide, wide), wide)]
            moves.append((
                pltpu.make_async_copy(src, held.at[j], read.at[j]),
                pltpu.make_async_copy(held.at[j], to, written.at[j]),
            ))
        for r, _ in moves:
            r.start()
        for r, w in moves:
            r.wait()
            w.start()
        for _, w in moves:
            w.wait()


def block_call(x, wg, wu, wd):
    rows, d = x.shape
    ff = wg.shape[1]
    half, nb = d // 2, d // 8
    hw = nb // 2
    chunks = rows // CHUNK * 4
    dma, any_ = pltpu.SemaphoreType.DMA, pl.BlockSpec(memory_space=pl.ANY)
    flops = 6 * rows * d * ff
    summed, _, late = pl.pallas_call(
        kernel,
        out_shape=[
            jax.ShapeDtypeStruct((rows, d), BF16),
            jax.ShapeDtypeStruct((rows, half), BF16),
            jax.ShapeDtypeStruct((CHUNK, LATE * nb), BF16),
        ],
        in_specs=[any_] * 4,
        out_specs=[any_] * 3,
        scratch_shapes=[
            pltpu.VMEM((BLOCK, d), BF16),
            pltpu.VMEM((BLOCK, ff), BF16),
            pltpu.VMEM((DEEP, 2, d, NA), BF16),
            pltpu.VMEM((2, ff, nb), BF16),
            pltpu.VMEM((4, BLOCK, nb), F32),
            pltpu.VMEM((4, BLOCK, nb), BF16),
            pltpu.VMEM((BLOCK, nb), BF16),
            pltpu.VMEM((BLOCK, nb), BF16),
            pltpu.VMEM((2, 2, CHUNK, hw), BF16),
            pltpu.VMEM((SLOTS, CHUNK, hw), BF16),
            pltpu.VMEM((RING, CHUNK, hw), BF16),
            pltpu.VMEM((RING, CHUNK, hw), BF16),
            dma, dma((DEEP, 2)), dma((2,)), dma, dma, pltpu.SemaphoreType.REGULAR,
            dma((4,)), dma((2, chunks)), dma((RING,)), dma((SLOTS,)),
            dma((RING, 4)), dma((2, chunks)), dma, dma, dma, dma((2, 2)),
        ],
        compiler_params=pltpu.CompilerParams(collective_id=0, has_side_effects=True, vmem_limit_bytes=VMEM),
        cost_estimate=pl.CostEstimate(flops=flops, bytes_accessed=10**9, transcendentals=rows * ff),
        name="mlp_block",
    )(x, wg, wu, wd)

    wide = LATE * nb
    own = lax.ppermute(late, "tp", [(2, 0), (3, 1), (4, 6), (5, 7)])
    out = jax.ShapeDtypeStruct((rows, d), BF16)
    params = pltpu.CompilerParams(vmem_limit_bytes=VMEM)

    def copy_call(first, count, extra, alias, name):
        return pl.pallas_call(
            functools.partial(copy_rows, first, count),
            out_shape=out,
            in_specs=[any_] * (1 + len(extra)),
            out_specs=any_,
            scratch_shapes=[pltpu.VMEM((count, PIECE, d), BF16), dma((count,)), dma((count,))],
            input_output_aliases=alias,
            compiler_params=params,
            cost_estimate=pl.CostEstimate(flops=count * COPY_FLOPS, bytes_accessed=count * PIECE * d * 4, transcendentals=0),
            name=name,
        )(summed, *extra)

    own, y = lax.optimization_barrier((own, copy_call(0, FIRST, (), {}, "copy_first")))
    par = lax.ppermute(own, "tp", [(0, 1), (1, 0), (6, 7), (7, 6)])
    y = copy_call(FIRST, rows // PIECE - FIRST, (own, y), {2: 0}, "copy_rest")
    return pl.pallas_call(
        add_late,
        out_shape=out,
        in_specs=[any_] * 3,
        out_specs=any_,
        scratch_shapes=[pltpu.VMEM((2, CHUNK, wide), BF16), dma((2,)), dma((2,))],
        input_output_aliases={0: 0},
        compiler_params=params,
        name="late_chunks",
    )(y, own, par)


def solution(mesh):
    return jax.shard_map(
        block_call,
        mesh=mesh,
        in_specs=(P("dp", None), P(None, "tp"), P(None, "tp"), P("tp", None)),
        out_specs=P("dp", None),
        check_vma=False,
    )
```

```python
import functools

import jax
import jax.numpy as jnp
from jax import lax
from jax.experimental import pallas as pl
from jax.experimental.pallas import tpu as pltpu
from jax.sharding import PartitionSpec as P

MESH = pl.DeviceIdType.MESH
BF16, F32 = jnp.bfloat16, jnp.float32
BLOCK, CHUNK, NA = 384, 128, 256
BULK = 1
PIECE, FIRST, COPY_FLOPS = 16, 88, 125 * 10**6
LATE = 2
VMEM = 67043328
SLOTS, RING, DEEP = 8, 4, 3
STEP_A, STEP_B, DUE, TICK = 184, 144, 700, 270
TAIL_A, TAIL_B = 130, 94
LAGS, BEHIND = (0, 2, 5), 16


def kernel(
    x, wg, wu, wd,
    y, cin, late,
    xb, hb, wa, wb, part, sent, psend, pbuf, cload, xin, xsend, tsend,
    sx, sa, sb, p_send, p_recv, p_free, o_send, c_recv, x_send, x_recv,
    t_send, y_recv, f_send, g_send, yp_recv, l_sem,
):
    rows, d = x.shape
    ff = wg.shape[1]
    half, nb = d // 2, d // 8
    hw = nb // 2
    steps_a, whole, per = ff // NA, rows // BLOCK, BLOCK // CHUNK
    tail = rows - whole * BLOCK
    blocks, chunks, per_tail = whole + (tail > 0), rows // CHUNK * 4, max(tail // CHUNK, 1)
    tick = TICK

    dp, me = lax.axis_index("dp"), lax.axis_index("tp")
    z, c = me // 2, me % 2
    inner = (z == 1) | (z == 2)
    outer = jnp.logical_not(inner)
    partner = me + 1 - 2 * c
    inward = (1 + z // 2) * 2 + c
    outward = (3 * (z - 1)) * 2 + c
    across = (3 - z) * 2 + c
    mine = pl.multiple_of(jnp.where(z == 2, hw, 0), hw)
    other = pl.multiple_of(hw - mine, hw)
    near = pl.multiple_of(jnp.where(z == 3, hw, 0), hw)
    own0, par0 = c * half, (1 - c) * half

    def remote(src, dst, send, recv, to):
        return pltpu.make_async_remote_copy(
            src_ref=src, dst_ref=dst, send_sem=send, recv_sem=recv,
            device_id=(dp, to), device_id_type=MESH,
        )

    def place(u):
        b, w = lax.div(u, 4 * per), lax.rem(u, 4 * per)
        n = jnp.where(b < whole, per, per_tail)
        i = jnp.where(b < whole, lax.div(w, per), lax.div(w, per_tail))
        r = w - i * n
        return (
            pl.ds(pl.multiple_of(b * BLOCK + r * CHUNK, CHUNK), CHUNK), i, pl.ds(pl.multiple_of(r * CHUNK, CHUNK), CHUNK)
        )

    def cols(base, i, off, n):
        return pl.ds(pl.multiple_of(base + i * nb + off, n), n)

    def x_copy(b, m):
        return pltpu.make_async_copy(x.at[pl.ds(pl.multiple_of(b * BLOCK, CHUNK), m), :], xb.at[pl.ds(0, m), :], sx)

    def a_copies(n, s):
        col = pl.ds(pl.multiple_of(n * NA, NA), NA)
        return [pltpu.make_async_copy(w.at[:, col], wa.at[s, j], sa.at[s, j]) for j, w in enumerate((wg, wu))]

    def b_copy(base, i, s):
        return pltpu.make_async_copy(wd.at[:, cols(base, i, 0, nb)], wb.at[s], sb.at[s])

    def p_copy(m):
        return remote(psend.at[pl.ds(0, m), :], pbuf.at[pl.ds(0, m), :], p_send, p_recv, partner)

    def o_copies(b, i, r, u):
        rw = pl.ds(pl.multiple_of(b * BLOCK + r * CHUNK, CHUNK), CHUNK)
        return [
            remote(
                sent.at[i, pl.ds(r * CHUNK, CHUNK), pl.ds(off, hw)], cin.at[rw, cols(0, i, off, hw)],
                o_send.at[i], c_recv.at[j, u], inward,
            )
            for j, off in enumerate((pl.multiple_of(hw - near, hw), near))
        ]

    def o_wait(i, m):
        at = pl.ds(0, m)
        remote(sent.at[i, at, :], cin.at[at, cols(0, i, 0, nb)], o_send.at[i], c_recv.at[0, 0], inward).wait_send()

    def c_half(u, j):
        rw, i, _ = place(u)
        return cin.at[rw, cols(0, i, (other, mine)[j], hw)]

    def c_arrival(u, j):
        return remote(c_half(u, j), c_half(u, j), o_send.at[0], c_recv.at[j, u], outward)

    def c_load(u, j):
        s = lax.rem(u, 2)
        return pltpu.make_async_copy(c_half(u, j), cload.at[j, s], l_sem.at[j, s])

    def e_copy(u):
        return remote(xsend.at[lax.rem(u, RING)], xin.at[lax.rem(u, SLOTS)], x_send.at[lax.rem(u, RING)], x_recv.at[lax.rem(u, SLOTS)], across)

    def t_copies(u):
        rw, i, _ = place(u)
        dst, s = y.at[rw, cols(own0, i, mine, hw)], lax.rem(u, RING)
        src = tsend.at[s]
        return [
            remote(src, dst, t_send.at[s, 0], y_recv.at[0, u], outward),
            remote(src, dst, t_send.at[s, 1], y_recv.at[0, u], across),
            remote(src, dst, t_send.at[s, 2], yp_recv, partner),
            pltpu.make_async_copy(src, dst, t_send.at[s, 3]),
        ]

    def t_wait(u):
        near_copy, *others, here = t_copies(u)
        pl.when(u < chunks - LATE)(near_copy.wait_send)
        for t in others:
            t.wait_send()
        here.wait()

    def hand_on(u):
        rw, i, _ = place(u)
        at = y.at[rw, cols(own0, i, other, hw)]
        return remote(at, at, f_send, y_recv.at[1, u], outward), remote(at, at, g_send, yp_recv, partner)

    def pass_over(u):
        rw, i, _ = place(u)
        at = y.at[rw, cols(own0, i, 0, nb)]
        return remote(at, at, g_send, yp_recv, partner)

    def y_arrival(u, kind, off):
        rw, i, _ = place(u)
        at = y.at[rw, cols(own0, i, off, hw)]
        return remote(at, at, f_send, y_recv.at[kind, u], across)

    def advance(clock, step):
        t, due, *made = clock
        t = t + step
        on = jnp.where(t >= due, 1, 0)
        return (t, due + tick * on, made[0] + on, *made[:-1])

    def turn(clock, stage):
        made = clock[2:]
        lag, behind = (LAGS[stage], 0) if stage < 3 else (0, BEHIND)
        u = made[lag + 1] - behind
        return u, (made[lag] > made[lag + 1]) & (u >= 0) & (u < chunks - LATE * (stage == 3))

    def before(clock):
        def fetch(u, j):
            c_arrival(u, j).wait_recv()
            c_load(u, j).start()

        for j in (0, 1):
            u, on = turn(clock, j)
            pl.when(inner & on)(functools.partial(fetch, u, j))

    def add_outer(u):
        @pl.when(u >= RING)
        def _():
            e_copy(u - RING).wait_send()

        _, i, r = place(u)
        c_load(u, 0).wait()
        xsend[lax.rem(u, RING)] = (part[i, r, pl.ds(other, hw)] + cload[0, lax.rem(u, 2)].astype(F32)).astype(BF16)
        e_copy(u).start()

    def add_across(u):
        @pl.when(u >= RING)
        def _():
            t_wait(u - RING)

        _, i, r = place(u)
        c_load(u, 1).wait()
        here = part[i, r, pl.ds(mine, hw)] + cload[1, lax.rem(u, 2)].astype(F32)
        e_copy(u).wait_recv()
        tsend[lax.rem(u, RING)] = (here + xin[lax.rem(u, SLOTS)].astype(F32)).astype(BF16)
        near_copy, *others = t_copies(u)
        pl.when(u < chunks - LATE)(near_copy.start)
        for t in others:
            t.start()

    def pass_outward(u):
        y_arrival(u, 0, other).wait_recv()
        out, over = hand_on(u)
        pl.when(u < chunks - LATE)(out.start)
        over.start()

    def pass_across(u):
        y_arrival(u, 0, near).wait_recv()
        y_arrival(u, 1, pl.multiple_of(hw - near, hw)).wait_recv()
        pass_over(u).start()

    def after(clock):
        for stage, (role, work) in enumerate(
            ((inner, add_outer), (inner, add_across), (inner, pass_outward), (outer, pass_across))
        ):
            u, on = turn(clock, stage)
            pl.when(role & on)(functools.partial(work, u))

    x_copy(0, BLOCK).start(priority=BULK)
    for t in a_copies(0, 0):
        t.start(priority=BULK)

    barrier = pltpu.get_barrier_semaphore()
    pl.semaphore_signal(barrier, inc=1, device_id=(dp, partner), device_id_type=MESH)

    @pl.when(inner)
    def _():
        pl.semaphore_signal(barrier, inc=1, device_id=(dp, outward), device_id_type=MESH)
        pl.semaphore_signal(barrier, inc=1, device_id=(dp, across), device_id_type=MESH)

    @pl.when(outer)
    def _():
        pl.semaphore_signal(barrier, inc=1, device_id=(dp, inward), device_id_type=MESH)

    def next_x(b):
        @pl.when(b + 1 < whole)
        def _():
            x_copy(b + 1, BLOCK).start(priority=BULK)

        if tail:
            @pl.when(b + 1 == whole)
            def _():
                x_copy(b + 1, tail).start(priority=BULK)

    def block(b, m, clock, long_a, long_b):
        x_copy(b, m).wait()
        mine_rows = pl.ds(0, m)

        for n in range(1, DEEP - 1):
            for t in a_copies(n, n):
                t.start(priority=BULK)

        def a_step(n, clock):
            s, clock = lax.rem(n, DEEP), advance(clock, long_a)

            @pl.when(n + DEEP - 1 < steps_a)
            def _():
                for t in a_copies(n + DEEP - 1, lax.rem(n + DEEP - 1, DEEP)):
                    t.start(priority=BULK)

            @pl.when(n == steps_a - 1)
            def _():
                b_copy(par0, 0, 0).start(priority=BULK)
                b_copy(own0, 0, 1).start(priority=BULK)

            @pl.when((b == 0) & (n == steps_a - 1) & inner)
            def _():
                pl.semaphore_wait(barrier, 3)

            @pl.when((b == 0) & (n == steps_a - 1) & outer)
            def _():
                pl.semaphore_wait(barrier, 2)

            before(clock)
            for t in a_copies(n, s):
                t.wait()
            gate = jnp.dot(xb[mine_rows, :], wa[s, 0], preferred_element_type=F32)
            up = jnp.dot(xb[mine_rows, :], wa[s, 1], preferred_element_type=F32)
            hb[mine_rows, pl.ds(pl.multiple_of(n * NA, NA), NA)] = (jax.nn.silu(gate) * up).astype(BF16)
            after(clock)
            return clock

        clock = lax.fori_loop(0, steps_a, a_step, clock)
        next_x(b)

        def b_step(i, clock):
            clock, count = advance(clock, long_b), b * 4 + i
            b_copy(par0, i, 0).wait()

            @pl.when((count > 0) & (i > 0))
            def _():
                p_copy(m).wait_send()

            @pl.when((count > 0) & (i == 0))
            def _():
                p_copy(BLOCK).wait_send()

            before(clock)
            psend[mine_rows, :] = jnp.dot(hb[mine_rows, :], wb[0], preferred_element_type=F32).astype(BF16)

            @pl.when(count > 0)
            def _():
                pl.semaphore_wait(p_free, 1)

            p_copy(m).start()

            @pl.when(i < 3)
            def _():
                b_copy(par0, i + 1, 0).start(priority=BULK)

            @pl.when((i == 3) & (b + 1 < blocks))
            def _():
                for t in a_copies(0, 0):
                    t.start(priority=BULK)

            after(clock)
            clock = advance(clock, long_b)
            before(clock)
            b_copy(own0, i, 1).wait()
            part[i, mine_rows, :] = jnp.dot(hb[mine_rows, :], wb[1], preferred_element_type=F32)

            @pl.when(i < 3)
            def _():
                b_copy(own0, i + 1, 1).start(priority=BULK)

            p_copy(m).wait_recv()

            @pl.when(inner)
            def _():
                part[i, mine_rows, :] += pbuf[mine_rows, :].astype(F32)

            @pl.when(outer)
            def _():
                @pl.when(b > 0)
                def _():
                    o_wait(i, BLOCK)

                for r in range(m // CHUNK):
                    at = pl.ds(r * CHUNK, CHUNK)
                    sent[i, at, :] = (part[i, at, :] + pbuf[at, :].astype(F32)).astype(BF16)
                    for o in o_copies(b, i, r, b * 4 * per + i * (m // CHUNK) + r):
                        o.start()

            @pl.when(count < blocks * 4 - 1)
            def _():
                pl.semaphore_signal(p_free, inc=1, device_id=(dp, partner), device_id_type=MESH)

            after(clock)
            return clock

        return lax.fori_loop(0, 4, b_step, clock)

    clock = (-steps_a * STEP_A, DUE) + (0,) * (max(LAGS) + 2)
    clock = lax.fori_loop(0, whole, lambda b, clock: block(b, BLOCK, clock, STEP_A, STEP_B), tuple(jnp.int32(v) for v in clock))
    if tail:
        clock = block(whole, tail, clock, TAIL_A, TAIL_B)

    def drain(_, clock):
        clock = advance(clock, tick)
        before(clock)
        after(clock)
        return clock

    end = (whole - 1) * (steps_a * STEP_A + 8 * STEP_B) + 8 * STEP_B + (tail > 0) * (steps_a * TAIL_A + 8 * TAIL_B)
    left = chunks + max(BEHIND, max(LAGS)) - (end - DUE) // tick
    lax.fori_loop(0, left, drain, clock)

    p_copy(tail or BLOCK).wait_send()

    def bytes_of(count, columns):
        return y.at[pl.ds(0, count * CHUNK * columns // d), :]

    early = chunks - LATE

    @pl.when(outer)
    def _():
        for i in range(4):
            o_wait(i, tail or BLOCK)
        passed = bytes_of(early, nb)
        remote(passed, passed, g_send, yp_recv, partner).wait_send()
        remote(passed, passed, g_send, yp_recv, partner).wait_recv()

    @pl.when(inner)
    def _():
        for s in range(RING):
            e_copy(chunks - RING + s).wait_send()
            t_wait(chunks - RING + s)
        out, over, took = bytes_of(early, hw), bytes_of(chunks, hw), bytes_of(chunks, nb)
        remote(out, out, f_send, yp_recv, partner).wait_send()
        remote(over, over, g_send, yp_recv, partner).wait_send()
        remote(took, took, g_send, yp_recv, partner).wait_recv()
        moves = []
        for s in range(late.shape[1] // hw):
            src = y.at[pl.ds(rows - CHUNK, CHUNK), pl.ds(pl.multiple_of(own0 + half - late.shape[1] + s * hw, hw), hw)]
            moves.append((
                pltpu.make_async_copy(src, tsend.at[s], t_send.at[s, 0]),
                pltpu.make_async_copy(tsend.at[s], late.at[:, pl.ds(s * hw, hw)], t_send.at[s, 1]),
            ))
        for read, _ in moves:
            read.start()
        for read, write in moves:
            read.wait()
            write.start()
        for _, write in moves:
            write.wait()


def copy_rows(first, count, src, *refs):
    dst, held, read, written = refs[-4:]

    def move(k):
        rows = pl.ds((first + k) * PIECE, PIECE)
        return (
            pltpu.make_async_copy(src.at[rows, :], held.at[k], read.at[k]),
            pltpu.make_async_copy(held.at[k], dst.at[rows, :], written.at[k]),
        )

    for k in range(count):
        move(k)[0].start()
    for k in range(count):
        move(k)[0].wait()
        move(k)[1].start()
    for k in range(count):
        move(k)[1].wait()


def add_late(y_in, own, par, y, held, read, written):
    rows, d = y.shape
    me = lax.axis_index("tp")
    z, c = me // 2, me % 2
    wide = own.shape[1]

    @pl.when((z == 0) | (z == 3))
    def _():
        moves = []
        for j, (src, side) in enumerate(((own, c), (par, 1 - c))):
            to = y.at[pl.ds(rows - CHUNK, CHUNK), pl.ds(pl.multiple_of(side * (d // 2) + d // 2 - wide, wide), wide)]
            moves.append((
                pltpu.make_async_copy(src, held.at[j], read.at[j]),
                pltpu.make_async_copy(held.at[j], to, written.at[j]),
            ))
        for r, _ in moves:
            r.start()
        for r, w in moves:
            r.wait()
            w.start()
        for _, w in moves:
            w.wait()


def block_call(x, wg, wu, wd):
    rows, d = x.shape
    ff = wg.shape[1]
    half, nb = d // 2, d // 8
    hw = nb // 2
    chunks = rows // CHUNK * 4
    dma, any_ = pltpu.SemaphoreType.DMA, pl.BlockSpec(memory_space=pl.ANY)
    flops = 6 * rows * d * ff
    summed, _, late = pl.pallas_call(
        kernel,
        out_shape=[
            jax.ShapeDtypeStruct((rows, d), BF16),
            jax.ShapeDtypeStruct((rows, half), BF16),
            jax.ShapeDtypeStruct((CHUNK, LATE * nb), BF16),
        ],
        in_specs=[any_] * 4,
        out_specs=[any_] * 3,
        scratch_shapes=[
            pltpu.VMEM((BLOCK, d), BF16),
            pltpu.VMEM((BLOCK, ff), BF16),
            pltpu.VMEM((DEEP, 2, d, NA), BF16),
            pltpu.VMEM((2, ff, nb), BF16),
            pltpu.VMEM((4, BLOCK, nb), F32),
            pltpu.VMEM((4, BLOCK, nb), BF16),
            pltpu.VMEM((BLOCK, nb), BF16),
            pltpu.VMEM((BLOCK, nb), BF16),
            pltpu.VMEM((2, 2, CHUNK, hw), BF16),
            pltpu.VMEM((SLOTS, CHUNK, hw), BF16),
            pltpu.VMEM((RING, CHUNK, hw), BF16),
            pltpu.VMEM((RING, CHUNK, hw), BF16),
            dma, dma((DEEP, 2)), dma((2,)), dma, dma, pltpu.SemaphoreType.REGULAR,
            dma((4,)), dma((2, chunks)), dma((RING,)), dma((SLOTS,)),
            dma((RING, 4)), dma((2, chunks)), dma, dma, dma, dma((2, 2)),
        ],
        compiler_params=pltpu.CompilerParams(collective_id=0, has_side_effects=True, vmem_limit_bytes=VMEM),
        cost_estimate=pl.CostEstimate(flops=flops, bytes_accessed=10**9, transcendentals=rows * ff),
        name="mlp_block",
    )(x, wg, wu, wd)

    wide = LATE * nb
    own = lax.ppermute(late, "tp", [(2, 0), (3, 1), (4, 6), (5, 7)])
    out = jax.ShapeDtypeStruct((rows, d), BF16)
    params = pltpu.CompilerParams(vmem_limit_bytes=VMEM)

    def copy_call(first, count, extra, alias, name):
        return pl.pallas_call(
            functools.partial(copy_rows, first, count),
            out_shape=out,
            in_specs=[any_] * (1 + len(extra)),
            out_specs=any_,
            scratch_shapes=[pltpu.VMEM((count, PIECE, d), BF16), dma((count,)), dma((count,))],
            input_output_aliases=alias,
            compiler_params=params,
            cost_estimate=pl.CostEstimate(flops=count * COPY_FLOPS, bytes_accessed=count * PIECE * d * 4, transcendentals=0),
            name=name,
        )(summed, *extra)

    own, y = lax.optimization_barrier((own, copy_call(0, FIRST, (), {}, "copy_first")))
    par = lax.ppermute(own, "tp", [(0, 1), (1, 0), (6, 7), (7, 6)])
    y = copy_call(FIRST, rows // PIECE - FIRST, (own, y), {2: 0}, "copy_rest")
    return pl.pallas_call(
        add_late,
        out_shape=out,
        in_specs=[any_] * 3,
        out_specs=any_,
        scratch_shapes=[pltpu.VMEM((2, CHUNK, wide), BF16), dma((2,)), dma((2,))],
        input_output_aliases={0: 0},
        compiler_params=params,
        name="late_chunks",
    )(y, own, par)


def solution(mesh):
    return jax.shard_map(
        block_call,
        mesh=mesh,
        in_specs=(P("dp", None), P(None, "tp"), P(None, "tp"), P("tp", None)),
        out_specs=P("dp", None),
        check_vma=False,
    )
```
